32 devices in a mesh: vp: 32 (over z, y, x, core).
Axes of the slice: x: 2, y: 2, z: 4, core: 2. Of those that a mesh axis runs over, the one named last changes fastest.
Arguments:
- table_in: float32 [49152, 576], P('vp')
- table_out: float32 [49152, 576], P('vp')
- center_ids: int32 [131072], P('vp')
- context_ids: int32 [131072], P('vp')
- negative_ids: int32 [65536], P('vp')
Outputs:
- output 1: float32 [49152, 576], P('vp')
- output 2: float32 [49152, 576], P('vp')
All inputs are finite; a program needn't handle non-finite values.
Results may differ from the reference program's by a relative error of at most 0.001.
Values sent between devices are 32-bit elements.
A program may use at most 1 GiB of HBM per device.

```python
import jax
import jax.numpy as jnp
from jax import lax

VOCAB_SIZE = 49152
EMBED_DIM = 576
PAIRS_DEV = 4096
NEGATIVES = 2048
SHARDS = 32
ROWS_SHARD = VOCAB_SIZE // SHARDS
NEG_WEIGHT = 5.0
LEARN_RATE = 1.0
NEG_SCALE = NEG_WEIGHT / NEGATIVES


def draw_ids(base_key, num_ids):
    common_slots = 3 * num_ids // SHARDS
    common_rows = common_slots // 4
    span_rows = ROWS_SHARD - common_rows
    key_common, key_start, key_perm = jax.random.split(base_key, 3)
    slot_idx = jnp.arange(num_ids, dtype=jnp.int32)
    common_pick = jax.random.randint(key_common, (SHARDS, num_ids), 0, common_rows, dtype=jnp.int32)
    common_part = jnp.where(slot_idx < common_rows, slot_idx, common_pick)
    other_idx = jnp.maximum(slot_idx - common_slots, 0)
    shard_idx = other_idx % SHARDS
    rank_idx = other_idx // SHARDS
    starts = jax.random.randint(key_start, (SHARDS, SHARDS), 0, span_rows, dtype=jnp.int32)
    other_part = shard_idx * ROWS_SHARD + common_rows + (starts[:, shard_idx] + rank_idx) % span_rows
    id_table = jnp.where(slot_idx < common_slots, common_part, other_part)
    return jax.random.permutation(key_perm, id_table, axis=1, independent=True).reshape(-1)


def setup_inputs(seed: int = 0) -> dict:
    base_key = jax.random.key(seed)
    key_in, key_out, key_center, key_context, key_neg = jax.random.split(base_key, 5)
    row_scale = EMBED_DIM ** -0.25
    table_in = jax.random.normal(key_in, (VOCAB_SIZE, EMBED_DIM), jnp.float32) * row_scale
    table_out = jax.random.normal(key_out, (VOCAB_SIZE, EMBED_DIM), jnp.float32) * row_scale
    return {'table_in': table_in, 'table_out': table_out, 'center_ids': draw_ids(key_center, PAIRS_DEV), 'context_ids': draw_ids(key_context, PAIRS_DEV), 'negative_ids': draw_ids(key_neg, NEGATIVES)}


def reference(table_in, table_out, center_ids, context_ids, negative_ids):
    zero_table = jnp.zeros((VOCAB_SIZE, EMBED_DIM), jnp.float32)

    def scan_body(state_in, batch_ids):
        grad_in, grad_out = state_in
        center_row, context_row, negative_row = batch_ids
        center_vec = jnp.take(table_in, center_row, axis=0)
        context_vec = jnp.take(table_out, context_row, axis=0)
        negative_vec = jnp.take(table_out, negative_row, axis=0)
        pos_score = jnp.sum(center_vec * context_vec, axis=1)
        center_half = center_vec.astype(jnp.bfloat16)
        negative_half = negative_vec.astype(jnp.bfloat16)
        neg_score = jnp.dot(center_half, negative_half.T, preferred_element_type=jnp.float32)
        pos_grad = (jax.nn.sigmoid(pos_score) - 1.0)[:, None]
        neg_grad = (NEG_SCALE * jax.nn.sigmoid(neg_score)).astype(jnp.bfloat16)
        d_center = pos_grad * context_vec + jnp.dot(neg_grad, negative_half, preferred_element_type=jnp.float32)
        d_context = pos_grad * center_vec
        d_negative = jnp.dot(neg_grad.T, center_half, preferred_element_type=jnp.float32)
        grad_in = grad_in.at[center_row].add(d_center)
        grad_out = grad_out.at[context_row].add(d_context).at[negative_row].add(d_negative)
        return (grad_in, grad_out), None

    start_state = (zero_table, zero_table)
    batches = (center_ids.reshape(SHARDS, PAIRS_DEV), context_ids.reshape(SHARDS, PAIRS_DEV), negative_ids.reshape(SHARDS, NEGATIVES))
    grad_in, grad_out = lax.scan(scan_body, start_state, batches)[0]
    return (table_in - LEARN_RATE * grad_in, table_out - LEARN_RATE * grad_out)
```

```python
import jax
import jax.numpy as jnp
from jax import lax
from jax.sharding import PartitionSpec as P


LEARN_RATE = 1.0
NEG_WEIGHT = 5.0
AXIS_NAME = 'vp'
PLANE = 8
POS_BITS = 13
CELL_BITS = 14
NO_KEY = 2 ** 30
LANES = 128


def distinct_capacity(num_ids, shards):
    common_slots = 3 * num_ids // shards
    return common_slots // 4 + (num_ids - common_slots + shards - 1) // shards


def plan_list(id_list, shard_rows, lines, capacity):
    num_ids = id_list.shape[0]
    column_rows = lines * shard_rows
    shard_idx = id_list // shard_rows
    peer = shard_idx % PLANE
    row_key = peer * column_rows + (shard_idx // PLANE) * shard_rows + id_list % shard_rows
    packed = lax.sort((row_key << POS_BITS) | jnp.arange(num_ids, dtype=jnp.int32), is_stable=False)
    key_sorted = packed >> POS_BITS
    slot_sorted = packed & (2 ** POS_BITS - 1)
    is_first = jnp.concatenate([jnp.ones((1,), bool), key_sorted[1:] != key_sorted[:-1]])
    rank = jnp.cumsum(is_first.astype(jnp.int32)) - 1
    peer_sorted = key_sorted // column_rows
    below = (peer_sorted[None, :] < jnp.arange(PLANE + 1, dtype=jnp.int32)[:, None]) & is_first[None, :]
    start = jnp.sum(below.astype(jnp.int32), axis=1)
    start_sorted = jnp.sum(jnp.where(peer_sorted[None, :] == jnp.arange(PLANE, dtype=jnp.int32)[:, None], start[:PLANE, None], 0), axis=0)
    cell_sorted = peer_sorted * capacity + rank - start_sorted
    cell_of_id = lax.sort((slot_sorted << CELL_BITS) | cell_sorted, is_stable=False) & (2 ** CELL_BITS - 1)
    distinct = jnp.pad(lax.sort(jnp.where(is_first, key_sorted, NO_KEY), is_stable=False), (0, capacity))
    place = jnp.arange(capacity, dtype=jnp.int32)
    asks = []
    for p in range(PLANE):
        row = lax.dynamic_slice(distinct, (start[p],), (capacity,)) - p * column_rows
        asks.append(jnp.where(place < start[p + 1] - start[p], row, place))
    return cell_of_id, jnp.stack(asks)


def pair_grads(center_vec, context_vec, negative_vec):
    neg_scale = NEG_WEIGHT / negative_vec.shape[0]
    pos_score = jnp.sum(center_vec * context_vec, axis=1)
    center_half = center_vec.astype(jnp.bfloat16)
    negative_half = negative_vec.astype(jnp.bfloat16)
    neg_score = lax.dot_general(center_half, negative_half, (((1,), (1,)), ((), ())), preferred_element_type=jnp.float32)
    pos_grad = (jax.nn.sigmoid(pos_score) - 1.0)[:, None]
    neg_grad = (neg_scale * jax.nn.sigmoid(neg_score)).astype(jnp.bfloat16)
    d_center = pos_grad * context_vec + jnp.dot(neg_grad, negative_half, preferred_element_type=jnp.float32)
    d_context = pos_grad * center_vec
    d_negative = lax.dot_general(neg_grad, center_half, (((0,), (0,)), ((), ())), preferred_element_type=jnp.float32)
    return d_center, d_context, d_negative


def widen(shard, width):
    return jnp.pad(shard, ((0, 0), (0, width - shard.shape[1])))


def take_rows(table, rows):
    return table.at[rows].get(mode='promise_in_bounds')


def add_rows(num_rows, rows, values):
    return jnp.zeros((num_rows, values.shape[1]), values.dtype).at[rows].add(values, mode='promise_in_bounds')


def solution(mesh):
    shards = mesh.shape[AXIS_NAME]
    lines = shards // PLANE
    plane_groups = [[line * PLANE + q for q in range(PLANE)] for line in range(lines)]
    line_groups = [[line * PLANE + q for line in range(lines)] for q in range(PLANE)]

    def exchange(cells):
        return lax.all_to_all(cells, AXIS_NAME, 0, 0, axis_index_groups=plane_groups)

    def gather_lines(shard):
        return lax.all_gather(shard, AXIS_NAME, axis_index_groups=line_groups, tiled=True)

    def sum_lines(column):
        return lax.psum_scatter(column, AXIS_NAME, scatter_dimension=0, axis_index_groups=line_groups, tiled=True)

    def device_step(in_shard, out_shard, center_ids, context_ids, negative_ids):
        shard_rows, dim = in_shard.shape
        wide = -(-dim // LANES) * LANES
        pairs_dev = center_ids.shape[0]
        column_rows = lines * shard_rows
        cap_in = lines * distinct_capacity(pairs_dev, shards)
        cap_out = cap_in + lines * distinct_capacity(negative_ids.shape[0], shards)
        out_column = gather_lines(widen(out_shard, wide))
        out_cell, out_asks = plan_list(jnp.concatenate([context_ids, negative_ids]), shard_rows, lines, cap_out)
        in_column = gather_lines(widen(in_shard, wide))
        in_cell, in_asks = plan_list(center_ids, shard_rows, lines, cap_in)
        asked = exchange(jnp.concatenate([out_asks, in_asks], axis=1))
        out_asked = asked[:, :cap_out].reshape(-1)
        in_asked = asked[:, cap_out:].reshape(-1)
        out_found = take_rows(out_column, out_asked).reshape(PLANE, cap_out, wide)
        out_rows = exchange(out_found).reshape(-1, wide)
        in_found = take_rows(in_column, in_asked).reshape(PLANE, cap_in, wide)
        in_rows = exchange(in_found).reshape(-1, wide)
        looked_up = take_rows(out_rows, out_cell)
        center_vec = take_rows(in_rows, in_cell)
        d_center, d_context, d_negative = pair_grads(center_vec, looked_up[:pairs_dev], looked_up[pairs_dev:])
        in_cells = add_rows(PLANE * cap_in, in_cell, d_center)
        in_back = exchange(in_cells.reshape(PLANE, cap_in, wide)).reshape(-1, wide)
        out_cells = add_rows(PLANE * cap_out, out_cell, jnp.concatenate([d_context, d_negative]))
        out_back = exchange(out_cells.reshape(PLANE, cap_out, wide)).reshape(-1, wide)
        in_sum = sum_lines(add_rows(column_rows, in_asked, in_back))
        out_sum = sum_lines(add_rows(column_rows, out_asked, out_back))
        return in_shard - LEARN_RATE * in_sum[:, :dim], out_shard - LEARN_RATE * out_sum[:, :dim]

    return jax.shard_map(device_step, mesh=mesh, in_specs=(P(AXIS_NAME, None), P(AXIS_NAME, None), P(AXIS_NAME), P(AXIS_NAME), P(AXIS_NAME)), out_specs=(P(AXIS_NAME, None), P(AXIS_NAME, None)), check_vma=False)
```

```python
import functools

import jax
import jax.numpy as jnp
from jax import lax
from jax.experimental import pallas as pl
from jax.experimental.pallas import tpu as pltpu
from jax.sharding import PartitionSpec as P


LEARN_RATE = 1.0
NEG_WEIGHT = 5.0
AXIS_NAME = 'vp'
PLANE = 8
POS_BITS = 13
CELL_BITS = 14
NO_KEY = 2 ** 30
LANES = 128
CUTS = (0, 128, 384)
CHUNKS = range(len(CUTS))
PAIR_BLOCK = 512


def distinct_capacity(num_ids, shards):
    common_slots = 3 * num_ids // shards
    return common_slots // 4 + (num_ids - common_slots + shards - 1) // shards


def plan_list(id_list, shard_rows, lines, capacity):
    num_ids = id_list.shape[0]
    column_rows = lines * shard_rows
    shard_idx = id_list // shard_rows
    peer = shard_idx % PLANE
    row_key = peer * column_rows + (shard_idx // PLANE) * shard_rows + id_list % shard_rows
    packed = lax.sort((row_key << POS_BITS) | jnp.arange(num_ids, dtype=jnp.int32), is_stable=False)
    key_sorted = packed >> POS_BITS
    slot_sorted = packed & (2 ** POS_BITS - 1)
    is_first = jnp.concatenate([jnp.ones((1,), bool), key_sorted[1:] != key_sorted[:-1]])
    rank = jnp.cumsum(is_first.astype(jnp.int32)) - 1
    peer_sorted = key_sorted // column_rows
    below = (peer_sorted[None, :] < jnp.arange(PLANE + 1, dtype=jnp.int32)[:, None]) & is_first[None, :]
    start = jnp.sum(below.astype(jnp.int32), axis=1)
    start_sorted = jnp.sum(jnp.where(peer_sorted[None, :] == jnp.arange(PLANE, dtype=jnp.int32)[:, None], start[:PLANE, None], 0), axis=0)
    cell_sorted = peer_sorted * capacity + rank - start_sorted
    cell_of_id = lax.sort((slot_sorted << CELL_BITS) | cell_sorted, is_stable=False) & (2 ** CELL_BITS - 1)
    distinct = jnp.pad(lax.sort(jnp.where(is_first, key_sorted, NO_KEY), is_stable=False), (0, capacity))
    place = jnp.arange(capacity, dtype=jnp.int32)
    asks = []
    for p in range(PLANE):
        row = lax.dynamic_slice(distinct, (start[p],), (capacity,)) - p * column_rows
        asks.append(jnp.where(place < start[p + 1] - start[p], row, place))
    return cell_of_id, jnp.stack(asks)


def pair_kernel(neg_scale, bounds, *refs):
    n = len(bounds)
    center, context, negative, d_center, d_context, d_negative = (refs[k * n:(k + 1) * n] for k in range(6))
    neg_half = refs[6 * n]

    @pl.when(pl.program_id(0) == 0)
    def _():
        for k, (lo, hi) in enumerate(bounds):
            neg_half[:, lo:hi] = negative[k][...].astype(jnp.bfloat16)
            d_negative[k][...] = jnp.zeros_like(d_negative[k])

    u = [r[...] for r in center]
    v = [r[...] for r in context]
    pos_score = sum(jnp.sum(a * b, axis=1, keepdims=True) for a, b in zip(u, v))
    pos_grad = jax.nn.sigmoid(pos_score) - 1.0
    center_half = jnp.concatenate([a.astype(jnp.bfloat16) for a in u], axis=1)
    neg_score = lax.dot_general(center_half, neg_half[...], (((1,), (1,)), ((), ())), preferred_element_type=jnp.float32)
    neg_grad = (neg_scale * jax.nn.sigmoid(neg_score)).astype(jnp.bfloat16)
    from_neg = jnp.dot(neg_grad, neg_half[...], preferred_element_type=jnp.float32)
    to_neg = lax.dot_general(neg_grad, center_half, (((0,), (0,)), ((), ())), preferred_element_type=jnp.float32)
    for k, (lo, hi) in enumerate(bounds):
        d_context[k][...] = pos_grad * u[k]
        d_center[k][...] = pos_grad * v[k] + from_neg[:, lo:hi]
        d_negative[k][...] += to_neg[:, lo:hi]


def pair_grads(center, looked_up):
    pairs, negs = center[0].shape[0], looked_up[0].shape[0] - center[0].shape[0]
    widths = [c.shape[1] for c in center]
    total, n = sum(widths), len(widths)
    bounds = [(sum(widths[:k]), sum(widths[:k + 1])) for k in range(n)]
    pair_specs = [pl.BlockSpec((PAIR_BLOCK, w), lambda i: (i, 0)) for w in widths]
    neg_in_specs = [pl.BlockSpec((negs, w), lambda i: (pairs // negs, 0)) for w in widths]
    neg_out_specs = [pl.BlockSpec((negs, w), lambda i: (0, 0)) for w in widths]
    shapes = [jax.ShapeDtypeStruct((m, w), jnp.float32) for m in (pairs, pairs, negs) for w in widths]
    grads = pl.pallas_call(
        functools.partial(pair_kernel, NEG_WEIGHT / negs, bounds),
        grid=(pairs // PAIR_BLOCK,),
        in_specs=pair_specs + pair_specs + neg_in_specs,
        out_specs=pair_specs + pair_specs + neg_out_specs,
        out_shape=shapes,
        scratch_shapes=[pltpu.VMEM((negs, total), jnp.bfloat16)],
        compiler_params=pltpu.CompilerParams(dimension_semantics=('arbitrary',), vmem_limit_bytes=60 * 2 ** 20),
        cost_estimate=pl.CostEstimate(flops=6 * pairs * negs * total, bytes_accessed=4 * total * (4 * pairs + 2 * negs), transcendentals=2 * pairs * negs),
    )(*center, *looked_up, *looked_up)
    return grads[:n], grads[n:2 * n], grads[2 * n:]


def column_chunks(shard):
    parts = [shard[:, lo:hi] for lo, hi in zip(CUTS, CUTS[1:] + (shard.shape[1],))]
    return [jnp.pad(x, ((0, 0), (0, -x.shape[1] % LANES))) for x in parts]


def take_rows(table, rows):
    return table.at[rows].get(mode='promise_in_bounds')


def add_rows(num_rows, *parts):
    total = jnp.zeros((num_rows, parts[0][1].shape[1]), parts[0][1].dtype)
    for rows, values in parts:
        total = total.at[rows].add(values, mode='promise_in_bounds')
    return total


FETCH_ORDER = [('out', k) for k in CHUNKS] + [('in', k) for k in reversed(CHUNKS)]
BACK_ORDER = FETCH_ORDER[::-1]


def solution(mesh):
    shards = mesh.shape[AXIS_NAME]
    lines = shards // PLANE
    plane_groups = [[line * PLANE + q for q in range(PLANE)] for line in range(lines)]
    line_groups = [[line * PLANE + q for line in range(lines)] for q in range(PLANE)]

    def exchange(cells):
        return lax.all_to_all(cells, AXIS_NAME, 0, 0, axis_index_groups=plane_groups)

    def gather_lines(shard):
        return lax.all_gather(shard, AXIS_NAME, axis_index_groups=line_groups, tiled=True)

    def sum_lines(column):
        return lax.psum_scatter(column, AXIS_NAME, scatter_dimension=0, axis_index_groups=line_groups, tiled=True)

    def device_step(in_shard, out_shard, center_ids, context_ids, negative_ids):
        shard_rows, dim = in_shard.shape
        pairs_dev = center_ids.shape[0]
        num_rows = lines * shard_rows
        cap_in = lines * distinct_capacity(pairs_dev, shards)
        cap_out = cap_in + lines * distinct_capacity(negative_ids.shape[0], shards)
        capacity = {'out': cap_out, 'in': cap_in}
        shard = {'out': column_chunks(out_shard), 'in': column_chunks(in_shard)}
        column = {}
        for side, k in FETCH_ORDER:
            column[side, k] = gather_lines(shard[side][k])
        out_cell, out_asks = plan_list(jnp.concatenate([context_ids, negative_ids]), shard_rows, lines, cap_out)
        in_cell, in_asks = plan_list(center_ids, shard_rows, lines, cap_in)
        asked_all = exchange(jnp.concatenate([out_asks, in_asks], axis=1))
        asked = {'out': asked_all[:, :cap_out].reshape(-1), 'in': asked_all[:, cap_out:].reshape(-1)}
        cell = {'out': out_cell, 'in': in_cell}
        looked_up = {}
        for side, k in FETCH_ORDER:
            found = take_rows(column[side, k], asked[side]).reshape(PLANE, capacity[side], -1)
            returned = exchange(found)
            looked_up[side, k] = take_rows(returned.reshape(-1, returned.shape[2]), cell[side])
        d_center, d_context, d_negative = pair_grads([looked_up['in', k] for k in CHUNKS], [looked_up['out', k] for k in CHUNKS])
        row_sum = {}
        for side, k in BACK_ORDER:
            parts = [(in_cell, d_center[k])] if side == 'in' else [(out_cell[:pairs_dev], d_context[k]), (out_cell[pairs_dev:], d_negative[k])]
            cells = add_rows(PLANE * capacity[side], *parts)
            arrived = exchange(cells.reshape(PLANE, capacity[side], -1))
            dense = add_rows(num_rows, (asked[side], arrived.reshape(-1, arrived.shape[2])))
            row_sum[side, k] = sum_lines(dense)
        new = []
        for side, old in (('in', in_shard), ('out', out_shard)):
            grad = jnp.concatenate([row_sum[side, k] for k in CHUNKS], axis=1)[:, :dim]
            new.append(old - LEARN_RATE * grad)
        return tuple(new)

    return jax.shard_map(device_step, mesh=mesh, in_specs=(P(AXIS_NAME, None), P(AXIS_NAME, None), P(AXIS_NAME), P(AXIS_NAME), P(AXIS_NAME)), out_specs=(P(AXIS_NAME, None), P(AXIS_NAME, None)), check_vma=False)
```

```python
import functools

import jax
import jax.numpy as jnp
from jax import lax
from jax.experimental import pallas as pl
from jax.experimental.pallas import tpu as pltpu
from jax.sharding import PartitionSpec as P


LEARN_RATE = 1.0
NEG_WEIGHT = 5.0
AXIS_NAME = 'vp'
PLANE = 8
POS_BITS = 13
CELL_BITS = 14
NO_KEY = 2 ** 30
LANES = 128
CUTS = (0, 128, 384)
CHUNKS = range(len(CUTS))
BACK_CUTS = {'in': (0, 256), 'out': (0, 128, 384)}
PAIR_BLOCK = 512


def distinct_capacity(num_ids, shards):
    common_slots = 3 * num_ids // shards
    return common_slots // 4 + (num_ids - common_slots + shards - 1) // shards


def plan_list(id_list, shard_rows, lines, capacity):
    num_ids = id_list.shape[0]
    column_rows = lines * shard_rows
    shard_idx = id_list // shard_rows
    peer = shard_idx % PLANE
    row_key = peer * column_rows + (shard_idx // PLANE) * shard_rows + id_list % shard_rows
    packed = lax.sort((row_key << POS_BITS) | jnp.arange(num_ids, dtype=jnp.int32), is_stable=False)
    key_sorted = packed >> POS_BITS
    slot_sorted = packed & (2 ** POS_BITS - 1)
    is_first = jnp.concatenate([jnp.ones((1,), bool), key_sorted[1:] != key_sorted[:-1]])
    rank = jnp.cumsum(is_first.astype(jnp.int32)) - 1
    peer_sorted = key_sorted // column_rows
    below = (peer_sorted[None, :] < jnp.arange(PLANE + 1, dtype=jnp.int32)[:, None]) & is_first[None, :]
    start = jnp.sum(below.astype(jnp.int32), axis=1)
    start_sorted = jnp.sum(jnp.where(peer_sorted[None, :] == jnp.arange(PLANE, dtype=jnp.int32)[:, None], start[:PLANE, None], 0), axis=0)
    cell_sorted = peer_sorted * capacity + rank - start_sorted
    cell_of_id = lax.sort((slot_sorted << CELL_BITS) | cell_sorted, is_stable=False) & (2 ** CELL_BITS - 1)
    distinct = jnp.pad(lax.sort(jnp.where(is_first, key_sorted, NO_KEY), is_stable=False), (0, capacity))
    place = jnp.arange(capacity, dtype=jnp.int32)
    asks = []
    for p in range(PLANE):
        row = lax.dynamic_slice(distinct, (start[p],), (capacity,)) - p * column_rows
        asks.append(jnp.where(place < start[p + 1] - start[p], row, place))
    return cell_of_id, jnp.stack(asks)


def pair_kernel(neg_scale, counts, *refs):
    groups, at = [], 0
    for n in counts:
        groups.append(refs[at:at + n])
        at += n
    center, context, negative, d_center, d_out = groups
    neg_half, d_negative = refs[at:]
    step = pl.program_id(0)
    block = center[0].shape[0]
    blocks = pl.num_programs(0) - d_negative.shape[0] // block

    def put(chunks, values):
        lo = 0
        for c in chunks:
            c[...] = values[:, lo:lo + c.shape[1]]
            lo += c.shape[1]

    @pl.when(step == 0)
    def _():
        neg_half[...] = jnp.concatenate([r[...].astype(jnp.bfloat16) for r in negative], axis=1)
        d_negative[...] = jnp.zeros_like(d_negative)

    @pl.when(step < blocks)
    def _():
        u = jnp.concatenate([r[...] for r in center], axis=1)
        v = jnp.concatenate([r[...] for r in context], axis=1)
        pos_grad = jax.nn.sigmoid(jnp.sum(u * v, axis=1, keepdims=True)) - 1.0
        center_half = u.astype(jnp.bfloat16)
        neg_score = lax.dot_general(center_half, neg_half[...], (((1,), (1,)), ((), ())), preferred_element_type=jnp.float32)
        neg_grad = (neg_scale * jax.nn.sigmoid(neg_score)).astype(jnp.bfloat16)
        put(d_center, pos_grad * v + jnp.dot(neg_grad, neg_half[...], preferred_element_type=jnp.float32))
        put(d_out, pos_grad * u)
        d_negative[...] += lax.dot_general(neg_grad, center_half, (((0,), (0,)), ((), ())), preferred_element_type=jnp.float32)

    @pl.when(step >= blocks)
    def _():
        put(d_out, d_negative[pl.ds(pl.multiple_of((step - blocks) * block, block), block), :])


def pair_grads(center, looked_up):
    pairs, rows = center[0].shape[0], looked_up[0].shape[0]
    negs = rows - pairs
    widths = [c.shape[1] for c in center]
    total = sum(widths)
    back = {side: chunk_widths(BACK_CUTS[side], total) for side in ('in', 'out')}
    last = pairs // PAIR_BLOCK - 1
    specs = [pl.BlockSpec((PAIR_BLOCK, w), lambda i: (jnp.minimum(i, last), 0)) for w in widths]
    neg_specs = [pl.BlockSpec((negs, w), lambda i: (pairs // negs, 0)) for w in widths]
    in_specs = [pl.BlockSpec((PAIR_BLOCK, w), lambda i: (jnp.minimum(i, last), 0)) for w in back['in']]
    out_specs = [pl.BlockSpec((PAIR_BLOCK, w), lambda i: (i, 0)) for w in back['out']]
    grads = pl.pallas_call(
        functools.partial(pair_kernel, NEG_WEIGHT / negs, [len(widths)] * 3 + [len(back['in']), len(back['out'])]),
        grid=(rows // PAIR_BLOCK,),
        in_specs=specs + specs + neg_specs,
        out_specs=in_specs + out_specs,
        out_shape=[jax.ShapeDtypeStruct((m, w), jnp.float32) for side, m in (('in', pairs), ('out', rows)) for w in back[side]],
        scratch_shapes=[pltpu.VMEM((negs, total), jnp.bfloat16), pltpu.VMEM((negs, total), jnp.float32)],
        compiler_params=pltpu.CompilerParams(dimension_semantics=('arbitrary',), vmem_limit_bytes=60 * 2 ** 20),
        cost_estimate=pl.CostEstimate(flops=6 * pairs * negs * total, bytes_accessed=4 * total * (4 * pairs + 2 * negs), transcendentals=2 * pairs * negs),
    )(*center, *looked_up, *looked_up)
    return {'in': grads[:len(back['in'])], 'out': grads[len(back['in']):]}


def chunk_widths(cuts, total):
    return [hi - lo for lo, hi in zip(cuts, cuts[1:] + (total,))]


def column_chunks(shard):
    parts = [shard[:, lo:hi] for lo, hi in zip(CUTS, CUTS[1:] + (shard.shape[1],))]
    return [jnp.pad(x, ((0, 0), (0, -x.shape[1] % LANES))) for x in parts]


def take_rows(table, rows):
    return table.at[rows].get(mode='promise_in_bounds')


def add_rows(num_rows, rows, values):
    return jnp.zeros((num_rows, values.shape[1]), values.dtype).at[rows].add(values, mode='promise_in_bounds')


FETCH_ORDER = [('out', k) for k in CHUNKS] + [('in', k) for k in reversed(CHUNKS)]
BACK_ORDER = [('in', k) for k in range(len(BACK_CUTS['in']))] + [('out', k) for k in reversed(range(len(BACK_CUTS['out'])))]


def solution(mesh):
    shards = mesh.shape[AXIS_NAME]
    lines = shards // PLANE
    plane_groups = [[line * PLANE + q for q in range(PLANE)] for line in range(lines)]
    line_groups = [[line * PLANE + q for line in range(lines)] for q in range(PLANE)]

    def exchange(cells):
        return lax.all_to_all(cells, AXIS_NAME, 0, 0, axis_index_groups=plane_groups)

    def gather_lines(shard):
        return lax.all_gather(shard, AXIS_NAME, axis_index_groups=line_groups, tiled=True)

    def sum_lines(column):
        return lax.psum_scatter(column, AXIS_NAME, scatter_dimension=0, axis_index_groups=line_groups, tiled=True)

    def device_step(in_shard, out_shard, center_ids, context_ids, negative_ids):
        shard_rows, dim = in_shard.shape
        pairs_dev = center_ids.shape[0]
        num_rows = lines * shard_rows
        cap_in = lines * distinct_capacity(pairs_dev, shards)
        cap_out = cap_in + lines * distinct_capacity(negative_ids.shape[0], shards)
        capacity = {'out': cap_out, 'in': cap_in}
        shard = {'out': column_chunks(out_shard), 'in': column_chunks(in_shard)}
        column = {}
        for side, k in FETCH_ORDER:
            column[side, k] = gather_lines(shard[side][k])
        out_cell, out_asks = plan_list(jnp.concatenate([context_ids, negative_ids]), shard_rows, lines, cap_out)
        in_cell, in_asks = plan_list(center_ids, shard_rows, lines, cap_in)
        asked_all = exchange(jnp.concatenate([out_asks, in_asks], axis=1))
        asked = {'out': asked_all[:, :cap_out].reshape(-1), 'in': asked_all[:, cap_out:].reshape(-1)}
        cell = {'out': out_cell, 'in': in_cell}
        looked_up = {}
        for side, k in FETCH_ORDER:
            found = take_rows(column[side, k], asked[side]).reshape(PLANE, capacity[side], -1)
            returned = exchange(found)
            looked_up[side, k] = take_rows(returned.reshape(-1, returned.shape[2]), cell[side])
        grads = pair_grads([looked_up['in', k] for k in CHUNKS], [looked_up['out', k] for k in CHUNKS])
        row_sum = {}
        for side, k in BACK_ORDER:
            cells = add_rows(PLANE * capacity[side], cell[side], grads[side][k])
            arrived = exchange(cells.reshape(PLANE, capacity[side], -1))
            dense = add_rows(num_rows, asked[side], arrived.reshape(-1, arrived.shape[2]))
            row_sum[side, k] = sum_lines(dense)
        new = []
        for side, old in (('in', in_shard), ('out', out_shard)):
            grad = jnp.concatenate([row_sum[side, k] for k in range(len(BACK_CUTS[side]))], axis=1)[:, :dim]
            new.append(old - LEARN_RATE * grad)
        return tuple(new)

    return jax.shard_map(device_step, mesh=mesh, in_specs=(P(AXIS_NAME, None), P(AXIS_NAME, None), P(AXIS_NAME), P(AXIS_NAME), P(AXIS_NAME)), out_specs=(P(AXIS_NAME, None), P(AXIS_NAME, None)), check_vma=False)
```
